32 devices in a mesh: section: 4 (over x, core), ep: 8 (over z, y).
Axes of the slice: x: 2, y: 2, z: 4, core: 2. Of those that a mesh axis runs over, the one named last changes fastest.
Arguments:
- output_grad: bfloat16 [4, 2048, 1024], P('section', 'ep'), may hold values from -6 to 6
- layer_input: bfloat16 [4, 2048, 1024], P('section', 'ep'), may hold values from -6 to 6
- expert_ids: int32 [4, 2048, 8], P('section', 'ep'), may hold values from 0 to 31, all different within a row; in each aligned block of 256 rows (0 to 255, 256 to 511, ..., all dimensions but the last counted through in order) at most 80 rows name the same one
- route_probs: bfloat16 [4, 2048, 8], P('section', 'ep'), may hold values from 0.049804688 to 0.44921875
- gate_weight: bfloat16 [4, 32, 1024, 384], P('section', 'ep'), may hold values from -0.1875 to 0.1875
- up_weight: bfloat16 [4, 32, 1024, 384], P('section', 'ep'), may hold values from -0.1875 to 0.1875
- down_weight: bfloat16 [4, 32, 384, 1024], P('section', 'ep'), may hold values from -0.3125 to 0.3125
- saved_inputs: bfloat16 [4, 32, 640, 1024], P('section', 'ep'), may hold values from -6 to 6
- saved_gate_grad: bfloat16 [4, 32, 640, 384], P('section', 'ep'), may hold values from -0.5 to 0.5
- saved_up_grad: bfloat16 [4, 32, 640, 384], P('section', 'ep'), may hold values from -0.5 to 0.5
- saved_counts: int32 [4, 32, 8], P('section', 'ep'), may hold values from 0 to 80, as said below
Outputs:
- upstream_grad: bfloat16 [4, 2048, 1024], P('section', 'ep')
- prob_grad: bfloat16 [4, 2048, 8], P('section', 'ep')
- gate_weight_grad: bfloat16 [4, 32, 1024, 384], P('section', 'ep')
- up_weight_grad: bfloat16 [4, 32, 1024, 384], P('section', 'ep')
The draws below stay inside these ranges and needn't reach their ends.
Inputs may be any that keep to these rules, and one draw needn't show every extreme that they name: `expert_ids`: each token names 8 different experts. Among the tokens of one device (aligned blocks of 256 tokens of a section) no expert is named more than 80 times, a bound that some block reaches. `saved_counts`: rows of a block at or beyond its count are padding; some block is full in every draw.
All inputs are finite; a program needn't handle non-finite values.
Results may differ from the reference program's by a relative error of at most 0.008.
Values may be sent and summed in bfloat16 or wider, within the bound.
A program may use at most 128 MiB of HBM per device.

```python
import math
import jax
import jax.numpy as jnp
import numpy as np
from jax import lax

D = 1024
FF = 384
TOP = 8
TOK_DEV = 256
SECTIONS = 4
TOKENS = 2048
EXPERTS = 32
SOURCES = 8
CAP = 80
SLOTS = 640
N_EP = 8


def draw_saved_counts(key, part):
    base = jax.random.randint(jax.random.fold_in(key, 11), (SECTIONS, EXPERTS, SOURCES), 0, CAP + 1)
    chosen = jax.random.randint(jax.random.fold_in(key, 12), (SECTIONS, 1, 1), 0, EXPERTS * SOURCES)
    flat = jnp.arange(EXPERTS * SOURCES, dtype=jnp.int32).reshape(1, EXPERTS, SOURCES)
    return jnp.where(flat == chosen, CAP, base).astype(jnp.int32)


def block_scale(rng, shape, shards, least, high):
    factor_of, own = 1.0, jax.random.fold_in(rng, 6)
    for axis_at, blocks in shards:
        draws = jnp.exp(jax.random.uniform(jax.random.fold_in(own, axis_at), (blocks,), jnp.float32, least / len(shards), high / len(shards)))
        factor_of = factor_of * jnp.repeat(draws, shape[axis_at] // blocks).reshape([-1 if axis == axis_at else 1 for axis in range(len(shape))])
    return factor_of


def deal_out(key, own, number, rows, amount, top, reach, slope):
    sequence = jax.random.permutation(key, amount)
    packed, common = shares(amount, rows * top, reach, slope, True), shares(amount, rows * top, reach, slope, False)
    places = jnp.arange(amount)

    def named(sizes, rotation):
        used = int((sizes > 0).sum())
        fixed = max(1, used // 4)
        passed = fixed + (places - fixed + rotation * (used - fixed)) % max(1, amount - fixed)
        return jnp.zeros((amount,), jnp.int32).at[sequence[jnp.where(places < fixed, places, passed)]].set(jnp.asarray(sizes, jnp.int32))

    sizes = jnp.where(number % 4 == 0, named(packed, number // 4), named(common, number - number // 4 - 1))
    mixed = jax.random.permutation(jax.random.fold_in(own, 3), amount)
    giver, receiver = mixed[0:amount // 2 * 2:2], mixed[1:amount // 2 * 2:2]
    slack = jnp.minimum(sizes[giver] - 1, reach - sizes[receiver]) // 2
    slack = jnp.where((giver == sequence[0]) | (receiver == sequence[0]) | (sizes[receiver] == 0), 0, jnp.maximum(slack, 0))
    passed = jax.random.randint(jax.random.fold_in(own, 4), (amount // 2,), 0, 1 << 20) % (slack + 1)
    sizes = sizes.at[giver].add(-passed).at[receiver].add(passed)
    labels = jnp.searchsorted(jnp.cumsum(sizes), jnp.arange(rows * top), side="right").astype(jnp.int32)
    grid = labels.reshape(top, rows).T
    grid = grid[jax.random.permutation(jax.random.fold_in(own, 1), rows)]
    rotation = jax.random.randint(jax.random.fold_in(own, 2), (rows, 1), 0, top)
    return jnp.take_along_axis(grid, (jnp.arange(top)[None, :] + rotation) % top, axis=1)


def shares(amount, total, limit, skew, full):
    weights = [(1 << 20) // math.isqrt(rank ** skew) + 1 for rank in range(1, amount + 1)]
    largest = limit if full else min(limit, max(-(-total // amount), total * weights[0] // sum(weights)))
    least = 1 if total - largest >= amount - 1 else 0
    given, spare = [largest] + [least] * (amount - 1), total - largest - least * (amount - 1)
    while spare > 0:
        free = [i for i in range(1, amount) if given[i] < largest] or [i for i in range(1, amount) if given[i] < limit]
        whole, budget = sum([weights[i] for i in free]), spare
        for i in free:
            more = min(limit - given[i], max(1, budget * weights[i] // whole), spare)
            given[i] = given[i] + more
            spare = spare - more
    return np.array(given)


def scatter_about(key, shape, deviation, reach, pieces=(), held_as=jnp.bfloat16):
    values = jax.random.normal(key, shape, jnp.float32) * deviation
    if len(pieces) > 0:
        values = block_scale(key, shape, pieces, -0.22, 0.18) * values
    return jnp.clip(values, min=-reach, max=reach).astype(held_as)


def setup_inputs(seed: int = 0) -> dict:
    splits = jax.random.split(jax.random.key(seed), 12)
    output_grad = scatter_about(splits[0], (SECTIONS, TOKENS, D), 1.0, 6.0, ((0, 4), (1, 8)))
    layer_input = scatter_about(splits[1], (SECTIONS, TOKENS, D), 1.0, 6.0, ((0, 4), (1, 8)))
    expert_ids_keys = jax.random.split(jax.random.fold_in(splits[2], 1), SECTIONS * TOKENS // TOK_DEV)
    expert_ids_turns = jax.random.permutation(jax.random.fold_in(splits[2], 3), SECTIONS * TOKENS // TOK_DEV)
    expert_ids = jax.vmap(lambda own, number: deal_out(jax.random.fold_in(splits[2], 2), own, number, TOK_DEV, EXPERTS, TOP, CAP, 2))(expert_ids_keys, expert_ids_turns).reshape((SECTIONS, TOKENS, TOP))
    route_probs = jnp.clip(0.049804688 + 0.39941406 * jax.random.uniform(splits[3], (SECTIONS, TOKENS, TOP), jnp.float32) ** block_scale(splits[3], (SECTIONS, TOKENS, TOP), ((0, 4), (1, 8)), -0.2, 0.2), 0.049804688, 0.44921875).astype(jnp.bfloat16)
    gate_weight = scatter_about(splits[4], (SECTIONS, EXPERTS, D, FF), D ** -0.5, 0.1875, ((0, 4), (1, 8)))
    up_weight = scatter_about(splits[5], (SECTIONS, EXPERTS, D, FF), D ** -0.5, 0.1875, ((0, 4), (1, 8)))
    down_weight = scatter_about(splits[6], (SECTIONS, EXPERTS, FF, D), FF ** -0.5, 0.3125, ((0, 4), (1, 8)))
    saved_inputs = scatter_about(splits[7], (SECTIONS, EXPERTS, SLOTS, D), 1.0, 6.0, ((0, 4), (1, 8)))
    saved_gate_grad = scatter_about(splits[8], (SECTIONS, EXPERTS, SLOTS, FF), 0.0625, 0.5, ((0, 4), (1, 8)))
    saved_up_grad = scatter_about(splits[9], (SECTIONS, EXPERTS, SLOTS, FF), 0.0625, 0.5, ((0, 4), (1, 8)))
    saved_counts = draw_saved_counts(jax.random.fold_in(splits[11], 71), 0)
    return {"output_grad": output_grad, "layer_input": layer_input, "expert_ids": expert_ids, "route_probs": route_probs, "gate_weight": gate_weight, "up_weight": up_weight, "down_weight": down_weight, "saved_inputs": saved_inputs, "saved_gate_grad": saved_gate_grad, "saved_up_grad": saved_up_grad, "saved_counts": saved_counts}


def block_slots(block_ids):
    flat_ids = block_ids.reshape(-1)
    onehot = (flat_ids[:, None] == jnp.arange(EXPERTS, dtype=jnp.int32)[None, :]).astype(jnp.int32)
    before = jnp.cumsum(onehot, axis=0) - onehot
    return jnp.sum(before * onehot, axis=1).astype(jnp.int32)


def expert_backward(operands):
    grad_rows, input_rows, prob_rows, w_gate, w_up, w_down = operands
    gate_pre = jnp.dot(input_rows, w_gate, preferred_element_type=jnp.float32)
    up_pre = jnp.dot(input_rows, w_up, preferred_element_type=jnp.float32)
    sigma = jax.nn.sigmoid(gate_pre)
    active = gate_pre * sigma
    hidden = (active * up_pre).astype(jnp.bfloat16)
    hidden_grad = jnp.dot(grad_rows, w_down.T, preferred_element_type=jnp.float32)
    output_rows = jnp.dot(hidden, w_down, preferred_element_type=jnp.float32)
    slot_prob = jnp.sum(output_rows * grad_rows.astype(jnp.float32), axis=1).astype(jnp.bfloat16)
    scaled = hidden_grad * prob_rows.astype(jnp.float32)[:, None]
    gate_grad = (scaled * up_pre * sigma * (1.0 + gate_pre * (1.0 - sigma))).astype(jnp.bfloat16)
    up_grad = (scaled * active).astype(jnp.bfloat16)
    slot_grad = jnp.dot(gate_grad, w_gate.T, preferred_element_type=jnp.float32)
    slot_grad = slot_grad + jnp.dot(up_grad, w_up.T, preferred_element_type=jnp.float32)
    return slot_grad.astype(jnp.bfloat16), slot_prob


def weight_pair(operands):
    masked, gate_grad, up_grad = operands
    gate_part = jnp.dot(masked.T, gate_grad, preferred_element_type=jnp.float32).astype(jnp.bfloat16)
    up_part = jnp.dot(masked.T, up_grad, preferred_element_type=jnp.float32).astype(jnp.bfloat16)
    return gate_part, up_part


def section_pass(grad, inputs, ids, probs, w_gate, w_up, w_down):
    blocks = ids.reshape(N_EP, TOK_DEV * TOP)
    slots = jax.vmap(block_slots)(blocks)
    source = jnp.arange(N_EP, dtype=jnp.int32)[:, None]
    place = (blocks * SLOTS + source * CAP + slots).reshape(-1).astype(jnp.int32)
    token = (jnp.arange(TOKENS * TOP, dtype=jnp.int32) // TOP).astype(jnp.int32)
    grad_rows = jnp.zeros((EXPERTS * SLOTS, D), jnp.bfloat16).at[place].set(grad[token])
    input_rows = jnp.zeros((EXPERTS * SLOTS, D), jnp.bfloat16).at[place].set(inputs[token])
    prob_rows = jnp.zeros((EXPERTS * SLOTS,), jnp.bfloat16).at[place].set(probs.reshape(-1))
    slot_grad, slot_prob = lax.map(expert_backward, (grad_rows.reshape(EXPERTS, SLOTS, D), input_rows.reshape(EXPERTS, SLOTS, D), prob_rows.reshape(EXPERTS, SLOTS), w_gate, w_up, w_down))
    picked = slot_grad.reshape(EXPERTS * SLOTS, D)[place]
    input_grad = jnp.sum(picked.reshape(TOKENS, TOP, D).astype(jnp.float32), axis=1).astype(jnp.bfloat16)
    prob_part = slot_prob.reshape(-1)[place].reshape(TOKENS, TOP)
    return input_grad, prob_part


def weight_pass(inputs, gate_grad, up_grad, counts):
    capacity = jnp.arange(CAP, dtype=jnp.int32)
    live = (capacity[None, None, :] < counts[:, :, None]).reshape(EXPERTS, SLOTS)
    masked = inputs * live.astype(jnp.bfloat16)[:, :, None]
    return lax.map(weight_pair, (masked, gate_grad, up_grad))


def reference(output_grad, layer_input, expert_ids, route_probs, gate_weight, up_weight, down_weight, saved_inputs, saved_gate_grad, saved_up_grad, saved_counts):
    input_grads = []
    prob_grads = []
    gate_grads = []
    up_grads = []
    for section_index in range(SECTIONS):
        input_grad, prob_part = section_pass(output_grad[section_index], layer_input[section_index], expert_ids[section_index], route_probs[section_index], gate_weight[section_index], up_weight[section_index], down_weight[section_index])
        gate_part, up_part = weight_pass(saved_inputs[section_index], saved_gate_grad[section_index], saved_up_grad[section_index], saved_counts[section_index])
        input_grads.append(input_grad)
        prob_grads.append(prob_part)
        gate_grads.append(gate_part)
        up_grads.append(up_part)
    stacked = jnp.stack(input_grads)
    upstream_grad = jnp.concatenate([stacked[1:], jnp.zeros_like(stacked[:1])], axis=0)
    return upstream_grad, jnp.stack(prob_grads), jnp.stack(gate_grads), jnp.stack(up_grads)
```

```python
import functools

import jax
import jax.numpy as jnp
from jax import lax
from jax.experimental import pallas as pl
from jax.experimental.pallas import tpu as pltpu
from jax.sharding import PartitionSpec as P

F32 = jnp.float32
BF16 = jnp.bfloat16
MESH = pl.DeviceIdType.MESH
VMEM = pl.BlockSpec(memory_space=pltpu.VMEM)
SMEM = pl.BlockSpec(memory_space=pltpu.SMEM)
ANY = pl.BlockSpec(memory_space=pl.ANY)
TILE = 256


def guarded(when, act):
    if when is None:
        act()
    else:
        pl.when(when)(act)


def both(a, b):
    return jnp.logical_and(a, b)


def add(a, b):
    return (a.astype(F32) + b.astype(F32)).astype(BF16)


def dot(a, b, dims):
    return lax.dot_general(a, b, (dims, ((), ())), preferred_element_type=F32)


def cuts(width):
    return max(width * 3 // 1024, 1) * 128, max(width // 1024, 1) * 128


def fused_kernel(
    count, sections, cap,
    g, x, ids, probs, counts, gate_w, up_w, down_w, held_in, gate_in, up_in,
    out, prob_out, gate_out, up_out,
    x_all, g_all, s_all, w_in, w_down, held, gate_held, up_held, gate_stage, up_stage,
    slots, weights, rows, keep_hidden, keep_active, keep_gate, back, part, prob_part, prob_in,
    a_sum, a_side, a_take, b_sum, b_take, b_side, land_a, land_b,
    own_sem, load_sem, held_sem, stage_sem, s_send, s_recv, z_send, z_recv, y_send, y_recv,
    o_send, o_recv, p_send, p_recv, c_send, c_recv, line_send, line_recv, shift_send, shift_recv,
):
    me = lax.axis_index("ep")
    section = lax.axis_index("section")
    outer, inner = me // 2, me % 2
    other = 1 - inner
    line = count // 2
    up = ((outer + 1) % line) * 2 + inner
    down = ((outer + line - 1) % line) * 2 + inner
    sides = (up, down)
    partner = outer * 2 + other
    experts = gate_w.shape[0]
    tokens, width = g.shape
    hidden = gate_w.shape[2]
    top = ids.shape[0]
    padded = rows.shape[1] // 2
    slot_rows = held_in.shape[1]
    cut, low_cut = cuts(width)
    everything, few, many = pl.ds(0, width), pl.ds(0, cut), pl.ds(cut, width - cut)
    side_list = (0, 1)

    def remote(src, dst, send, recv, target):
        return pltpu.make_async_remote_copy(
            src_ref=src, dst_ref=dst, send_sem=send, recv_sem=recv, device_id=target,
            device_id_type=MESH,
        )

    own = [
        pltpu.make_async_copy(g, g_all.at[me], own_sem.at[0]),
        pltpu.make_async_copy(x, x_all.at[me], own_sem.at[1]),
    ]
    for copy in own:
        copy.start()

    def held_loads(expert, at):
        return [
            pltpu.make_async_copy(src.at[expert], dst.at[at], held_sem.at[kind, at])
            for kind, (src, dst) in enumerate(
                ((held_in, held), (gate_in, gate_held), (up_in, up_held))
            )
        ]

    for expert in range(min(2, experts)):
        for copy in held_loads(expert, expert):
            copy.start()
    loads = [
        pltpu.make_async_copy(gate_w, w_in.at[:, :, pl.ds(0, hidden)], load_sem.at[0]),
        pltpu.make_async_copy(up_w, w_in.at[:, :, pl.ds(hidden, hidden)], load_sem.at[1]),
        pltpu.make_async_copy(down_w, w_down, load_sem.at[2]),
    ]
    for copy in loads:
        copy.start()

    s_all[me] = jnp.concatenate([ids[...].astype(F32), probs[...].astype(F32)], axis=0).astype(BF16)

    barrier = pltpu.get_barrier_semaphore()
    for away in range(1, count):
        pl.semaphore_signal(
            barrier, inc=1, device_id={"ep": (me + away) % count}, device_id_type=MESH
        )
    for away in (1, sections - 1):
        pl.semaphore_signal(
            barrier, inc=1, device_id={"section": (section + away) % sections}, device_id_type=MESH
        )
    for copy in own:
        copy.wait()
    pl.semaphore_wait(barrier, count + 1)

    def s_copy(away):
        return remote(
            s_all.at[me], s_all.at[me], s_send.at[away - 1], s_recv.at[away - 1],
            {"ep": (me + away) % count},
        )

    for away in range(1, count):
        s_copy(away).start()

    def block(step, side):
        return (outer + (-step if side == 0 else step) + 2 * line) % line

    def arrives(step, side):
        return outer >= step + 1 if side == 0 else outer + step + 1 <= line - 1

    def leaves(step, side):
        if side == 0:
            return both(outer >= step, outer < line - 1)
        return both(outer + step <= line - 1, outer > 0)

    pieces = ((x_all, everything), (g_all, many), (g_all, few), (g_all, few))

    def z_copy(at, side, step):
        ref, columns = pieces[at]
        spot = ref.at[block(step, side) * 2 + (other if at == 3 else inner), :, columns]
        return remote(
            spot, spot, z_send.at[at, side, step], z_recv.at[at, side, step], {"ep": sides[side]}
        )

    def y_copy(at, side, step):
        ref, columns = pieces[at]
        spot = ref.at[block(step + 1, side) * 2 + inner, :, columns]
        return remote(
            spot, spot, y_send.at[at, side, step], y_recv.at[at, side, step], {"ep": partner}
        )

    def o_copy(at):
        ref, columns = pieces[at]
        spot = ref.at[me, :, columns]
        return remote(spot, spot, o_send.at[at], o_recv.at[at], {"ep": partner})

    o_copy(2).start()
    for at in range(3):
        for side in side_list:
            pl.when(leaves(0, side))(z_copy(at, side, 0).start)
    o_copy(0).start()
    o_copy(1).start()

    def weight_expert(expert, carry):
        at = expert % 2
        for copy in held_loads(expert, at):
            copy.wait()
        place = lax.broadcasted_iota(jnp.int32, (slot_rows, 128), 0)
        live = jnp.zeros((slot_rows, 128), F32)
        for source in range(count):
            low = source * cap
            inside = both(place >= low, place < low + counts[expert, source])
            live = jnp.where(inside, 1.0, live)
        live = live.astype(BF16)
        for ref in (gate_held, up_held):
            for group in range(hidden // 128):
                columns = pl.ds(group * 128, 128)
                ref[at, :, columns] = ref[at, :, columns] * live

        def stage_copies(old):
            return [
                pltpu.make_async_copy(stage.at[at], dst.at[old], stage_sem.at[kind, at])
                for kind, (stage, dst) in enumerate(((gate_stage, gate_out), (up_stage, up_out)))
            ]

        @pl.when(expert >= 2)
        def _():
            for copy in stage_copies(expert - 2):
                copy.wait()

        def body(tile, carry):
            columns = pl.ds(pl.multiple_of(tile * TILE, TILE), TILE)
            some = held[at, :, columns]
            for ref, stage in ((gate_held, gate_stage), (up_held, up_stage)):
                stage[at, columns, :] = dot(some, ref[at], ((0,), (0,))).astype(BF16)
            return carry

        lax.fori_loop(0, width // TILE, body, 0)
        for copy in stage_copies(expert):
            copy.start()

        @pl.when(expert + 2 < experts)
        def _():
            for copy in held_loads(expert + 2, at):
                copy.start()

        return carry

    def weight_finish():
        for expert in range(max(experts - 2, 0), experts):
            for kind, (stage, dst) in enumerate(((gate_stage, gate_out), (up_stage, up_out))):
                pltpu.make_async_copy(
                    stage.at[expert % 2], dst.at[expert], stage_sem.at[kind, expert % 2]
                ).wait()

    def route():
        members = []
        for source in range(count):
            named = s_all[source].astype(F32)
            chosen, prob = named[:top], named[top:]
            for expert in range(experts):
                hit = chosen == (me * experts + expert).astype(F32)
                members.append(jnp.max(jnp.where(hit, 1.0, 0.0), axis=0, keepdims=True))
                weights[source, expert] = jnp.sum(jnp.where(hit, prob, 0.0), axis=0, keepdims=True)
        member = jnp.concatenate(members, axis=0)
        earlier = lax.broadcasted_iota(jnp.int32, (tokens, tokens), 0) < lax.broadcasted_iota(
            jnp.int32, (tokens, tokens), 1
        )
        before = dot(
            member.astype(BF16), jnp.where(earlier, 1.0, 0.0).astype(BF16), ((1,), (0,))
        )
        slot = jnp.where(member > 0.5, before, -1.0)
        for source in range(count):
            for expert in range(experts):
                at = source * experts + expert
                slots[source, expert] = slot[at : at + 1]

    spots = lax.broadcasted_iota(jnp.int32, (padded, tokens), 0).astype(F32)

    def picked(source, scaled):
        parts = []
        for expert in range(experts):
            value = weights[source, expert] if scaled else 1.0
            parts.append(jnp.where(spots == slots[source, expert], value, 0.0).astype(BF16))
        return jnp.concatenate(parts, axis=0)

    def spread(unit, ref):
        for row in range(2):
            source = unit * 2 + row
            pick = picked(source, False)
            for tile in range(width // TILE):
                columns = pl.ds(tile * TILE, TILE)
                got = dot(pick, ref[source, :, columns], ((1,), (0,))).astype(BF16)
                for expert in range(experts):
                    rows[expert, pl.ds(row * padded, padded), columns] = got[
                        expert * padded : (expert + 1) * padded
                    ]

    def forward(unit, side):
        spread(unit, x_all)

        def body(expert, carry):
            pre = dot(rows[expert], w_in[expert], ((1,), (0,)))
            gate, upper = pre[:, :hidden], pre[:, hidden:]
            sigma = jax.nn.sigmoid(gate)
            active = gate * sigma
            keep_active[side, expert] = active
            keep_hidden[side, expert] = active * upper
            keep_gate[side, expert] = upper * sigma * (1.0 + gate * (1.0 - sigma))
            return carry

        lax.fori_loop(0, experts, body, 0)

    def backward(unit, side):
        spread(unit, g_all)

        def body(expert, carry):
            grad = dot(rows[expert], w_down[expert], ((1,), (1,)))
            score = jnp.sum(grad * keep_hidden[side, expert], axis=1, keepdims=True)
            score = score.astype(BF16).astype(F32)
            pre_grad = jnp.concatenate(
                [
                    (grad * keep_gate[side, expert]).astype(BF16),
                    (grad * keep_active[side, expert]).astype(BF16),
                ],
                axis=1,
            )
            for tile in range(width // TILE):
                columns = pl.ds(tile * TILE, TILE)
                sent = dot(pre_grad, w_in[expert, columns, :], ((1,), (1,))).astype(BF16)
                for row in range(2):
                    back[
                        row, pl.ds(pl.multiple_of(expert * padded, padded), padded), columns
                    ] = sent[row * padded : (row + 1) * padded]
            for row in range(2):
                source = unit * 2 + row
                mine = jnp.where(
                    spots == slots[source, expert], score[row * padded : (row + 1) * padded], 0.0
                )
                prob_part[source, expert] = jnp.sum(mine, axis=0, keepdims=True)
            return carry

        lax.fori_loop(0, experts, body, 0)
        for row in range(2):
            source = unit * 2 + row
            put = picked(source, True)
            for tile in range(width // TILE):
                columns = pl.ds(tile * TILE, TILE)
                part[source, :, columns] = dot(put, back[row, :, columns], ((0,), (0,))).astype(BF16)

    def valid(step, side):
        if side == 0:
            return outer >= step + 1
        return both(outer + step + 1 <= line - 1, step >= 0)

    def unit_loop(step, act, at):
        def body(side, carry):
            unit = (outer + jnp.where(side == 0, -step - 1, step + 1) + 2 * line) % line
            ok = jnp.where(
                side == 0,
                jnp.where(outer >= step + 1, 1, 0),
                jnp.where(both(outer + step + 1 <= line - 1, step >= 0), 1, 0),
            )

            @pl.when(ok == 1)
            def _():
                act(unit, side)

            return carry

        for side in side_list:
            @pl.when(both(valid(step, side), step >= 0))
            def _(side=side):
                y_copy(at, side, step).wait_recv()

        @pl.when(step < 0)
        def _():
            o_copy(at).wait_recv()

        lax.fori_loop(0, 2, body, 0)

    def take(at, step):
        for side in side_list:
            pl.when(arrives(step, side))(z_copy(at, side, step).wait_recv)

            @pl.when(both(leaves(step + 1, side), step < line - 2))
            def _(side=side):
                z_copy(at, side, step + 1).start()

            if at < 2:
                pl.when(arrives(step, side))(y_copy(at, side, step).start)

    def turn(index, carry):
        step = index - 1
        moving = both(step >= 0, step < line - 1)
        first = jnp.where(index == 0, 0, jnp.minimum(index + 1, experts))
        last = jnp.minimum(index + 2, experts)
        lax.fori_loop(first, last, weight_expert, 0)

        @pl.when(moving)
        def _():
            take(0, step)
            take(1, step)

        @pl.when(step >= 0)
        def _():
            unit_loop(step - 1, backward, 1)

        @pl.when(both(step >= 0, step < line - 2))
        def _():
            take(2, step)
            take(3, step)

        @pl.when(step < line - 1)
        def _():
            unit_loop(step, forward, 0)

        @pl.when(step == line - 2)
        def _():
            take(2, step)
            take(3, step)

        return carry

    for away in range(1, count):
        s_copy(away).wait_recv()
    o_copy(2).wait_recv()
    for side in side_list:
        pl.when(leaves(0, side))(z_copy(3, side, 0).start)
    route()
    for copy in loads:
        copy.wait()
    lax.fori_loop(0, line + 1, turn, 0)
    if experts > line + 2:
        lax.fori_loop(line + 2, experts, weight_expert, 0)

    low, high = pl.ds(0, low_cut), pl.ds(low_cut, width - low_cut)

    def goal(at):
        mixed = line - 1 - at // 2 if at % 2 == 0 else at // 2
        return jnp.where(outer == 0, line - 1 - at, jnp.where(outer == line - 1, at, mixed))

    def across(at):
        return remote(
            part.at[goal(at) * 2 + other, :, high], b_take.at[goal(at)], c_send.at[at],
            c_recv.at[at], {"ep": partner},
        )

    def p_copy(away):
        target = (me + away) % count
        return remote(
            prob_part.at[target], prob_in.at[me], p_send.at[away - 1], p_recv.at[away - 1],
            {"ep": target},
        )

    for at in range(line):
        across(at).start()
    for away in range(1, count):
        p_copy(away).start()
    prob_in[me] = prob_part[me]

    def line_copy(kind, source, side_ref, side, place, spot):
        return remote(
            source.at[place], side_ref.at[spot], line_send.at[kind, side, place],
            line_recv.at[kind, side, place], {"ep": sides[side]},
        )

    def spot_of(side, place, where):
        return jnp.where(place == where, line, place) if side == 1 else place

    def collect(kind, total, side_ref, side, place):
        spot = spot_of(side, place, outer)
        line_copy(kind, total, side_ref, side, place, spot).wait_recv()
        total[place] = add(total[place], side_ref[spot])

    def advance(kind, total, side_ref, place):
        @pl.when(both(place >= outer, outer > 0))
        def _():
            collect(kind, total, side_ref, 0, place)

        @pl.when(both(place <= outer, outer < line - 1))
        def _():
            collect(kind, total, side_ref, 1, place)

        @pl.when(place > outer)
        def _():
            line_copy(kind, total, side_ref, 0, place, spot_of(0, place, outer + 1)).start()

        @pl.when(place < outer)
        def _():
            line_copy(kind, total, side_ref, 1, place, spot_of(1, place, outer - 1)).start()

    a_across = remote(
        a_sum.at[0, outer], a_take, c_send.at[line], c_recv.at[line], {"ep": partner}
    )
    for at in range(line):
        place = goal(at)
        for kind, row in ((0, other), (1, inner)):
            a_sum[kind, place] = part[place * 2 + row, :, :low_cut]
            advance(kind, a_sum.at[kind], a_side.at[kind], place)
    a_across.start()
    for at in range(line):
        place = goal(at)
        across(at).wait_recv()
        b_sum[place] = add(b_take[place], part[place * 2 + inner, :, low_cut:])
        advance(2, b_sum, b_side, place)

    def shift(column, source, land):
        return remote(
            source, land, shift_send.at[column], shift_recv.at[column],
            {"section": (section + sections - 1) % sections},
        )

    a_across.wait_recv()
    a_sum[1, outer] = add(a_sum[1, outer], a_take[...])
    shifts = (shift(0, a_sum.at[1, outer], land_a), shift(1, b_sum.at[outer], land_b))

    @pl.when(section > 0)
    def _():
        for copy in shifts:
            copy.start()

    for away in range(1, count):
        p_copy(away).wait_recv()
    total = jnp.zeros((top, tokens), F32)
    for expert in range(experts * count):
        value = prob_in[expert // experts, expert % experts]
        total = jnp.where(ids[...] == expert, value, total)
    prob_out[...] = total.astype(BF16)
    weight_finish()

    for away in range(1, count):
        s_copy(away).wait_send()
        p_copy(away).wait_send()
    for at in range(3):
        o_copy(at).wait_send()

    def drain(step, carry):
        for side in side_list:
            for at in range(4):
                pl.when(leaves(step, side))(z_copy(at, side, step).wait_send)
            for at in range(2):
                pl.when(arrives(step, side))(y_copy(at, side, step).wait_send)
        return carry

    lax.fori_loop(0, line - 1, drain, 0)
    for at in range(line):
        across(at).wait_send()
    a_across.wait_send()
    for place in range(line):
        for kind, source, side_ref in (
            (0, a_sum.at[0], a_side.at[0]), (1, a_sum.at[1], a_side.at[1]), (2, b_sum, b_side),
        ):
            pl.when(place > outer)(line_copy(kind, source, side_ref, 0, place, place).wait_send)
            pl.when(place < outer)(line_copy(kind, source, side_ref, 1, place, place).wait_send)

    @pl.when(section > 0)
    def _():
        for copy in shifts:
            copy.wait_send()

    @pl.when(section < sections - 1)
    def _():
        shifts[0].wait_recv()
        out[:, :low_cut] = land_a[...]
        shifts[1].wait_recv()
        out[:, low_cut:] = land_b[...]

    @pl.when(section == sections - 1)
    def _():
        out[...] = jnp.zeros_like(out)


def fused(count, sections, g, x, ids, probs, counts, gate_w, up_w, down_w, held, gate, up):
    line = count // 2
    tokens, width = g.shape
    experts, _, hidden = gate_w.shape
    top = ids.shape[0]
    slot_rows = held.shape[1]
    cap = slot_rows // count
    padded = -(-cap // 16) * 16
    _, low_cut = cuts(width)
    rest = width - low_cut
    dma = pltpu.SemaphoreType.DMA
    grads = jax.ShapeDtypeStruct((experts, width, hidden), BF16)
    return pl.pallas_call(
        functools.partial(fused_kernel, count, sections, cap),
        out_shape=[
            jax.ShapeDtypeStruct((tokens, width), BF16),
            jax.ShapeDtypeStruct((top, tokens), BF16),
            grads,
            grads,
        ],
        in_specs=[ANY, ANY, VMEM, VMEM, SMEM] + [ANY] * 6,
        out_specs=[VMEM, VMEM, ANY, ANY],
        scratch_shapes=[
            pltpu.VMEM((count, tokens, width), BF16),
            pltpu.VMEM((count, tokens, width), BF16),
            pltpu.VMEM((count, 2 * top, tokens), BF16),
            pltpu.VMEM((experts, width, 2 * hidden), BF16),
            pltpu.VMEM((experts, hidden, width), BF16),
            pltpu.VMEM((2, slot_rows, width), BF16),
            pltpu.VMEM((2, slot_rows, hidden), BF16),
            pltpu.VMEM((2, slot_rows, hidden), BF16),
            pltpu.VMEM((2, width, hidden), BF16),
            pltpu.VMEM((2, width, hidden), BF16),
            pltpu.VMEM((count, experts, 1, tokens), F32),
            pltpu.VMEM((count, experts, 1, tokens), F32),
            pltpu.VMEM((experts, 2 * padded, width), BF16),
            pltpu.VMEM((2, experts, 2 * padded, hidden), F32),
            pltpu.VMEM((2, experts, 2 * padded, hidden), F32),
            pltpu.VMEM((2, experts, 2 * padded, hidden), F32),
            pltpu.VMEM((2, experts * padded, width), BF16),
            pltpu.VMEM((count, tokens, width), BF16),
            pltpu.VMEM((count, experts, 1, tokens), F32),
            pltpu.VMEM((count, experts, 1, tokens), F32),
            pltpu.VMEM((2, line, tokens, low_cut), BF16),
            pltpu.VMEM((2, line + 1, tokens, low_cut), BF16),
            pltpu.VMEM((tokens, low_cut), BF16),
            pltpu.VMEM((line, tokens, rest), BF16),
            pltpu.VMEM((line, tokens, rest), BF16),
            pltpu.VMEM((line + 1, tokens, rest), BF16),
            pltpu.VMEM((tokens, low_cut), BF16),
            pltpu.VMEM((tokens, rest), BF16),
            dma((2,)),
            dma((3,)),
            dma((3, 2)),
            dma((2, 2)),
            dma((count - 1,)),
            dma((count - 1,)),
            dma((4, 2, line - 1)),
            dma((4, 2, line - 1)),
            dma((2, 2, line - 1)),
            dma((2, 2, line - 1)),
            dma((3,)),
            dma((3,)),
            dma((count - 1,)),
            dma((count - 1,)),
            dma((line + 1,)),
            dma((line + 1,)),
            dma((3, 2, line)),
            dma((3, 2, line)),
            dma((2,)),
            dma((2,)),
        ],
        compiler_params=pltpu.CompilerParams(
            collective_id=0, has_side_effects=True, vmem_limit_bytes=63 * 1024 * 1024
        ),
    )(g, x, ids, probs, counts, gate_w, up_w, down_w, held, gate, up)


def publish_kernel(top, gate, up, out, gate_out, up_out, held, read, write):
    moves = []
    for source, goal in ((top, out), (gate, gate_out), (up, up_out)):
        half = source.shape[0] // 2
        for part in range(2):
            moves.append((source.at[pl.ds(part * half, half)], goal.at[pl.ds(part * half, half)]))
    spots = [held[at // 2].at[at % 2] for at in range(len(moves))]
    reads = [
        pltpu.make_async_copy(source, spot, read.at[at])
        for at, ((source, _), spot) in enumerate(zip(moves, spots))
    ]
    writes = [
        pltpu.make_async_copy(spot, goal, write.at[at])
        for at, ((_, goal), spot) in enumerate(zip(moves, spots))
    ]
    for copy in reads:
        copy.start()
    for before, after in zip(reads, writes):
        before.wait()
        after.start()
    for copy in writes:
        copy.wait()


def publish(top, gate, up):
    arrays = (top, gate, up)

    def kernel(a, b, c, d, e, f, h0, h1, h2, read, write):
        publish_kernel(a, b, c, d, e, f, (h0, h1, h2), read, write)

    return pl.pallas_call(
        kernel,
        out_shape=[jax.ShapeDtypeStruct(a.shape, a.dtype) for a in arrays],
        in_specs=[ANY] * 3,
        out_specs=[ANY] * 3,
        scratch_shapes=[
            pltpu.VMEM((2, a.shape[0] // 2) + a.shape[1:], a.dtype) for a in arrays
        ] + [pltpu.SemaphoreType.DMA((6,)), pltpu.SemaphoreType.DMA((6,))],
    )(*arrays)


def per_device(
    output_grad,
    layer_input,
    expert_ids,
    route_probs,
    gate_weight,
    up_weight,
    down_weight,
    saved_inputs,
    saved_gate_grad,
    saved_up_grad,
    saved_counts,
):
    upstream, prob, gate_part, up_part = fused(
        lax.axis_size("ep"),
        lax.axis_size("section"),
        output_grad[0],
        layer_input[0],
        expert_ids[0].T,
        route_probs[0].T,
        saved_counts[0],
        gate_weight[0],
        up_weight[0],
        down_weight[0],
        saved_inputs[0],
        saved_gate_grad[0],
        saved_up_grad[0],
    )
    upstream, gate_part, up_part = publish(upstream, gate_part, up_part)
    return (upstream[None], prob.T[None], gate_part[None], up_part[None])


def solution(mesh):
    three = P("section", "ep", None)
    four = P("section", "ep", None, None)
    return jax.shard_map(
        per_device,
        mesh=mesh,
        in_specs=(three, three, three, three, four, four, four, four, four, four, three),
        out_specs=(three, three, four, four),
        check_vma=False,
    )
```

```python
import functools

import jax
import jax.numpy as jnp
from jax import lax
from jax.experimental import pallas as pl
from jax.experimental.pallas import tpu as pltpu
from jax.sharding import PartitionSpec as P

F32 = jnp.float32
BF16 = jnp.bfloat16
MESH = pl.DeviceIdType.MESH
VMEM = pl.BlockSpec(memory_space=pltpu.VMEM)
SMEM = pl.BlockSpec(memory_space=pltpu.SMEM)
ANY = pl.BlockSpec(memory_space=pl.ANY)
HBM = pl.BlockSpec(memory_space=pltpu.HBM)
TILE = 256
PIECES = 2


def guarded(when, act):
    if when is None:
        act()
    else:
        pl.when(when)(act)


def both(a, b):
    return jnp.logical_and(a, b)


def add(a, b):
    return (a.astype(F32) + b.astype(F32)).astype(BF16)


def dot(a, b, dims):
    return lax.dot_general(a, b, (dims, ((), ())), preferred_element_type=F32)


def cut_of(width):
    return max(width * 5 // 1024, 1) * 128


def fused_kernel(
    count, sections, cap, roomy,
    g, x, ids, probs, counts, gate_w, up_w, down_w, held_in, gate_in, up_in,
    out, prob_out, gate_out, up_out,
    x_all, g_all, s_all, w_in, w_down, held, gate_held, up_held, gate_stage, up_stage,
    slots, weights, rows, keep_hidden, keep_active, keep_gate, back, part, prob_part, prob_in,
    chain_in, cross_in, end_in, end_sum, final_in,
    own_sem, load_sem, held_sem, stage_sem, s_send, s_recv, z_send, z_recv, y_send, y_recv,
    o_send, o_recv, p_send, p_recv, chain_send, chain_recv, cross_send, cross_recv, end_send,
    end_recv, final_send, final_recv, shift_send, shift_recv,
):
    me = lax.axis_index("ep")
    section = lax.axis_index("section")
    outer, inner = me // 2, me % 2
    other = 1 - inner
    line = count // 2
    up = ((outer + 1) % line) * 2 + inner
    down = ((outer + line - 1) % line) * 2 + inner
    sides = (up, down)
    partner = outer * 2 + other
    experts = gate_w.shape[0]
    tokens, width = g.shape
    hidden = gate_w.shape[2]
    top = ids.shape[0]
    padded = rows.shape[1] // 2
    slot_rows = held_in.shape[1]
    cut = cut_of(width)
    everything, few, many = pl.ds(0, width), pl.ds(0, cut), pl.ds(cut, width - cut)
    side_list = (0, 1)

    def remote(src, dst, send, recv, target):
        return pltpu.make_async_remote_copy(
            src_ref=src, dst_ref=dst, send_sem=send, recv_sem=recv, device_id=target,
            device_id_type=MESH,
        )

    own = [
        pltpu.make_async_copy(g, g_all.at[me], own_sem.at[0]),
        pltpu.make_async_copy(x, x_all.at[me], own_sem.at[1]),
    ]
    for copy in own:
        copy.start()

    def held_loads(expert, at):
        return [
            pltpu.make_async_copy(src.at[expert], dst.at[at], held_sem.at[kind, at])
            for kind, (src, dst) in enumerate(
                ((held_in, held), (gate_in, gate_held), (up_in, up_held))
            )
        ]

    s_all[me] = jnp.concatenate([ids[...].astype(F32), probs[...].astype(F32)], axis=0).astype(BF16)

    barrier = pltpu.get_barrier_semaphore()
    for away in range(1, count):
        pl.semaphore_signal(
            barrier, inc=1, device_id={"ep": (me + away) % count}, device_id_type=MESH
        )
    for away in (1, sections - 1):
        pl.semaphore_signal(
            barrier, inc=1, device_id={"section": (section + away) % sections}, device_id_type=MESH
        )
    pl.semaphore_wait(barrier, count + 1)

    def s_copy(away):
        return remote(
            s_all.at[me], s_all.at[me], s_send.at[away - 1], s_recv.at[away - 1],
            {"ep": (me + away) % count},
        )

    for away in range(1, count):
        s_copy(away).start()

    def block(step, side):
        return (outer + (-step if side == 0 else step) + 2 * line) % line

    def arrives(step, side):
        return outer >= step + 1 if side == 0 else outer + step + 1 <= line - 1

    def leaves(step, side):
        if side == 0:
            return both(outer >= step, outer < line - 1)
        return both(outer + step <= line - 1, outer > 0)

    pieces = ((x_all, everything), (g_all, many), (g_all, few), (g_all, few))

    def z_copy(at, side, step, source=None):
        ref, columns = pieces[at]
        spot = ref.at[block(step, side) * 2 + (other if at == 3 else inner), :, columns]
        return remote(
            spot if source is None else source.at[:, columns], spot, z_send.at[at, side, step],
            z_recv.at[at, side, step], {"ep": sides[side]},
        )

    def y_copy(at, side, step):
        ref, columns = pieces[at]
        spot = ref.at[block(step + 1, side) * 2 + inner, :, columns]
        return remote(
            spot, spot, y_send.at[at, side, step], y_recv.at[at, side, step], {"ep": partner}
        )

    def o_copy(at):
        ref, columns = pieces[at]
        spot = ref.at[me, :, columns]
        return remote(
            (x, g, g)[at].at[:, columns], spot, o_send.at[at], o_recv.at[at], {"ep": partner}
        )

    o_copy(2).start()
    for at in range(3):
        for side in side_list:
            pl.when(leaves(0, side))(z_copy(at, side, 0, (x, g, g)[at]).start)
    o_copy(0).start()
    o_copy(1).start()
    for expert in range(min(2, experts)):
        for copy in held_loads(expert, expert):
            copy.start()
    loads = [
        pltpu.make_async_copy(gate_w, w_in.at[:, :, pl.ds(0, hidden)], load_sem.at[0]),
        pltpu.make_async_copy(up_w, w_in.at[:, :, pl.ds(hidden, hidden)], load_sem.at[1]),
        pltpu.make_async_copy(down_w, w_down, load_sem.at[2]),
    ]
    for copy in loads:
        copy.start()


    def hop_of(side):
        return outer + 1 if side == 0 else outer - 1

    def chain(block_at, side, row, at, where):
        rows_at = pl.ds(at * (tokens // PIECES), tokens // PIECES)
        spot = jnp.where(block_at == where, line - 2, block_at - 1) if side == 1 else block_at - 1
        return remote(
            part.at[block_at * 2 + row, rows_at], chain_in.at[spot, row, rows_at],
            chain_send.at[block_at - 1, side, row, at], chain_recv.at[block_at - 1, side, row, at],
            {"ep": sides[side]},
        )

    def weight_expert(expert, carry):
        at = expert % 2
        for copy in held_loads(expert, at):
            copy.wait()
        place = lax.broadcasted_iota(jnp.int32, (slot_rows, 128), 0)
        live = jnp.zeros((slot_rows, 128), F32)
        for source in range(count):
            low = source * cap
            inside = both(place >= low, place < low + counts[expert, source])
            live = jnp.where(inside, 1.0, live)
        live = live.astype(BF16)
        for ref in (gate_held, up_held):
            for group in range(hidden // 128):
                columns = pl.ds(group * 128, 128)
                ref[at, :, columns] = ref[at, :, columns] * live

        def stage_copies(old):
            return [
                pltpu.make_async_copy(stage.at[at], dst.at[old], stage_sem.at[kind, at])
                for kind, (stage, dst) in enumerate(((gate_stage, gate_out), (up_stage, up_out)))
            ]

        if not roomy:
            @pl.when(expert >= 2)
            def _():
                for copy in stage_copies(expert - 2):
                    copy.wait()

        goals = (gate_out, up_out) if roomy else (gate_stage, up_stage)
        place_at = expert if roomy else at

        def body(tile, carry):
            columns = pl.ds(pl.multiple_of(tile * TILE, TILE), TILE)
            some = held[at, :, columns]
            for ref, stage in zip((gate_held, up_held), goals):
                stage[place_at, columns, :] = dot(some, ref[at], ((0,), (0,))).astype(BF16)
            return carry

        lax.fori_loop(0, width // TILE, body, 0)
        if not roomy:
            for copy in stage_copies(expert):
                copy.start()

        @pl.when(expert + 2 < experts)
        def _():
            for copy in held_loads(expert + 2, at):
                copy.start()

        return carry

    def weight_finish():
        if roomy:
            return
        for expert in range(max(experts - 2, 0), experts):
            for kind, (stage, dst) in enumerate(((gate_stage, gate_out), (up_stage, up_out))):
                pltpu.make_async_copy(
                    stage.at[expert % 2], dst.at[expert], stage_sem.at[kind, expert % 2]
                ).wait()

    def route():
        members = []
        for source in range(count):
            named = s_all[source].astype(F32)
            chosen, prob = named[:top], named[top:]
            for expert in range(experts):
                hit = chosen == (me * experts + expert).astype(F32)
                members.append(jnp.max(jnp.where(hit, 1.0, 0.0), axis=0, keepdims=True))
                weights[source, expert] = jnp.sum(jnp.where(hit, prob, 0.0), axis=0, keepdims=True)
        member = jnp.concatenate(members, axis=0)
        earlier = lax.broadcasted_iota(jnp.int32, (tokens, tokens), 0) < lax.broadcasted_iota(
            jnp.int32, (tokens, tokens), 1
        )
        before = dot(
            member.astype(BF16), jnp.where(earlier, 1.0, 0.0).astype(BF16), ((1,), (0,))
        )
        slot = jnp.where(member > 0.5, before, -1.0)
        for source in range(count):
            for expert in range(experts):
                at = source * experts + expert
                slots[source, expert] = slot[at : at + 1]

    spots = lax.broadcasted_iota(jnp.int32, (padded, tokens), 0).astype(F32)

    def picked(source, scaled):
        parts = []
        for expert in range(experts):
            value = weights[source, expert] if scaled else 1.0
            parts.append(jnp.where(spots == slots[source, expert], value, 0.0).astype(BF16))
        return jnp.concatenate(parts, axis=0)

    def spread(unit, ref):
        for row in range(2):
            source = unit * 2 + row
            pick = picked(source, False)
            for tile in range(width // TILE):
                columns = pl.ds(tile * TILE, TILE)
                got = dot(pick, ref[source, :, columns], ((1,), (0,))).astype(BF16)
                for expert in range(experts):
                    rows[expert, pl.ds(row * padded, padded), columns] = got[
                        expert * padded : (expert + 1) * padded
                    ]

    def forward(unit, side):
        spread(unit, x_all)

        def body(expert, carry):
            pre = dot(rows[expert], w_in[expert], ((1,), (0,)))
            gate, upper = pre[:, :hidden], pre[:, hidden:]
            sigma = jax.nn.sigmoid(gate)
            active = gate * sigma
            keep_active[side, expert] = active
            keep_hidden[side, expert] = active * upper
            keep_gate[side, expert] = upper * sigma * (1.0 + gate * (1.0 - sigma))
            return carry

        lax.fori_loop(0, experts, body, 0)

    def backward(unit, side):
        spread(unit, g_all)

        def body(expert, carry):
            grad = dot(rows[expert], w_down[expert], ((1,), (1,)))
            score = jnp.sum(grad * keep_hidden[side, expert], axis=1, keepdims=True)
            score = score.astype(BF16).astype(F32)
            pre_grad = jnp.concatenate(
                [
                    (grad * keep_gate[side, expert]).astype(BF16),
                    (grad * keep_active[side, expert]).astype(BF16),
                ],
                axis=1,
            )
            for tile in range(width // TILE):
                columns = pl.ds(tile * TILE, TILE)
                sent = dot(pre_grad, w_in[expert, columns, :], ((1,), (1,))).astype(BF16)
                for row in range(2):
                    back[
                        row, pl.ds(pl.multiple_of(expert * padded, padded), padded), columns
                    ] = sent[row * padded : (row + 1) * padded]
            for row in range(2):
                source = unit * 2 + row
                mine = jnp.where(
                    spots == slots[source, expert], score[row * padded : (row + 1) * padded], 0.0
                )
                prob_part[source, expert] = jnp.sum(mine, axis=0, keepdims=True)
            return carry

        lax.fori_loop(0, experts, body, 0)
        for row in range(2):
            source = unit * 2 + row
            put = picked(source, True)
            for tile in range(width // TILE):
                columns = pl.ds(tile * TILE, TILE)
                sent = dot(put, back[row, :, columns], ((0,), (0,)))
                part[source, :, columns] = sent.astype(BF16)
        within = both(unit > 0, unit < line - 1)
        for way, edge in ((0, 0), (1, line - 1)):
            @pl.when(both(outer == edge, within))
            def _(way=way, edge=edge):
                split = unit == (line - 2 if edge == 0 else 1)
                for at in range(PIECES):
                    for row in range(2):
                        send = chain(unit, way, row, at, hop_of(way)).start
                        if at < PIECES // 2:
                            send()
                        else:
                            pl.when(jnp.logical_not(split))(send)

    def unit_turn(step, side, act, at):
        unit = (outer + (-step - 1 if side == 0 else step + 1) + 2 * line) % line
        own_turn = step < 0
        later = both(arrives(step, side), step >= 0)
        pl.when(later)(y_copy(at, side, step).wait_recv)
        if side == 0:
            pl.when(own_turn)(o_copy(at).wait_recv)

        @pl.when(jnp.logical_or(later, own_turn) if side == 0 else later)
        def _():
            act(unit, side)

    def take(at, step):
        for side in side_list:
            pl.when(arrives(step, side))(z_copy(at, side, step).wait_recv)

            @pl.when(both(leaves(step + 1, side), step < line - 2))
            def _(side=side):
                z_copy(at, side, step + 1).start()

            if at < 2:
                pl.when(arrives(step, side))(y_copy(at, side, step).start)

    at_end = jnp.logical_or(outer == 0, outer == line - 1)

    def turn(index, carry):
        step = index - 1
        early = both(step >= 0, step < line - 2)
        pl.when(early)(lambda: take(0, step))
        pl.when(both(early, index == 1))(lambda: take(1, step))

        @pl.when(index < 2)
        def _():
            experts_of(index)

        @pl.when(step >= 0)
        def _():
            unit_turn(step - 1, 0, backward, 1)
            unit_turn(step - 1, 1, backward, 1)

        pl.when(both(early, index > 1))(lambda: take(1, step))

        @pl.when(index >= 2)
        def _():
            experts_of(index)

        @pl.when(step == line - 2)
        def _():
            take(0, step)
            take(1, step)
            chain_start(range(PIECES // 2, PIECES))

        @pl.when(early)
        def _():
            take(2, step)
            take(3, step)

        @pl.when(step < line - 1)
        def _():
            unit_turn(step, 0, forward, 0)
            unit_turn(step, 1, forward, 0)

        @pl.when(step == line - 2)
        def _():
            take(2, step)
            take(3, step)

        return carry

    def experts_of(index):
        first = jnp.where(index == 0, 0, jnp.minimum(index + 1, experts))
        last = jnp.minimum(index + 2, experts)
        lax.fori_loop(first, last, weight_expert, 0)

    def chain_start(some):
        for way, edge, unit in ((0, 0, line - 2), (1, line - 1, 1)):
            @pl.when(outer == edge)
            def _(way=way, unit=unit):
                for at in some:
                    for row in range(2):
                        chain(unit, way, row, at, hop_of(way)).start()

    for away in range(1, count):
        s_copy(away).wait_recv()
    route()
    for copy in own:
        copy.wait()
    o_copy(2).wait_recv()
    for side in side_list:
        pl.when(leaves(0, side))(z_copy(3, side, 0).start)
    for copy in loads:
        copy.wait()
    lax.fori_loop(0, line + 1, turn, 0)
    if experts > line + 2:
        lax.fori_loop(line + 2, experts, weight_expert, 0)

    span = tokens // PIECES
    far = jnp.where(outer < line // 2, line - 1, 0)
    near = line - 1 - far
    far_end, near_end = far // (line - 1), near // (line - 1)
    far_side = jnp.where(outer < line // 2, up, down)
    near_side = jnp.where(outer < line // 2, down, up)

    def chunk(at):
        return pl.ds(at * span, span)

    def p_copy(away):
        target = (me + away) % count
        return remote(
            prob_part.at[target], prob_in.at[me], p_send.at[away - 1], p_recv.at[away - 1],
            {"ep": target},
        )

    def cross(block_at, end, at):
        return remote(
            part.at[block_at * 2 + other, chunk(at)], cross_in.at[end, chunk(at)],
            cross_send.at[end, at], cross_recv.at[end, at], {"ep": partner},
        )

    def final(at):
        return remote(
            part.at[outer * 2 + other, chunk(at)], final_in.at[chunk(at)], final_send.at[at],
            final_recv.at[at], {"ep": partner},
        )

    def end_copy(end, at, target):
        return remote(
            end_sum.at[end, chunk(at)], end_in.at[end, chunk(at)], end_send.at[end, at],
            end_recv.at[end, at], {"ep": target},
        )

    def shift(source, at):
        return remote(
            source, out.at[chunk(at)], shift_send.at[at], shift_recv.at[at],
            {"section": (section + sections - 1) % sections},
        )

    for away in range(1, count):
        p_copy(away).start()
    prob_in[me] = prob_part[me]
    ends = ((far, far_end), (near, near_end))
    in_turn = [(end, at) for end in range(2) for at in range(PIECES)]
    mixed_up = [(end, at) for at in range(PIECES) for end in range(2)]

    def crossing(order):
        for end, piece in order:
            cross(*ends[end], piece).start()

    def end_step(order, place, target):
        is_far, at = order[place][0] == 0, order[place][1]
        block_at, end = ends[order[place][0]]
        cross(block_at, end, at).wait_recv()
        rows_at = chunk(at)
        total = part[block_at * 2 + inner, rows_at].astype(F32) + cross_in[end, rows_at].astype(F32)
        end_sum[end, rows_at] = total.astype(BF16)
        first = jnp.logical_or(outer == 0, outer == line - 1) if is_far else None

        def gather_in():
            end_copy(end, at, target).wait_recv()
            end_sum[end, rows_at] = add(end_sum[end, rows_at], end_in[end, rows_at])

        if is_far:
            pl.when(jnp.logical_not(first))(gather_in)
            end_copy(end, at, target).start()
        else:
            gather_in()

    @pl.when(at_end)
    def _():
        crossing(in_turn[:PIECES])
        for at in range(PIECES):
            end_step(in_turn, at, far_side)
        crossing(in_turn[PIECES:])
        for at in range(PIECES):
            end_step(in_turn, PIECES + at, near_side)

            @pl.when(section > 0)
            def _(at=at):
                shift(end_sum.at[near_end, chunk(at)], at).start()

    @pl.when(jnp.logical_not(at_end))
    def _():
        crossing(mixed_up)
        order = []
        for half in range((line - 1) // 2):
            order += [line - 2 - half] + ([1 + half] if 1 + half != line - 2 - half else [])
        for block_at in order:
            for side in side_list:
                @pl.when(block_at > outer if side == 0 else block_at < outer)
                def _(block_at=block_at, side=side):
                    for at in range(PIECES):
                        for row in range(2):
                            chain(block_at, side, row, at, outer).wait_recv()
                            spot = block_at * 2 + row
                            part[spot, chunk(at)] = add(
                                part[spot, chunk(at)], chain_in[block_at - 1, row, chunk(at)]
                            )
                            chain(block_at, side, row, at, hop_of(side)).start()
        for at in range(PIECES):
            end_step(mixed_up, 2 * at, far_side)
            end_step(mixed_up, 2 * at + 1, near_side)
            end_copy(near_end, at, near_side).start()
            for row in range(2):
                for side in side_list:
                    chain(outer, side, row, at, outer).wait_recv()
                spot = outer * 2 + row
                total = part[spot, chunk(at)].astype(F32)
                total = total + chain_in[outer - 1, row, chunk(at)].astype(F32)
                total = total + chain_in[line - 2, row, chunk(at)].astype(F32)
                part[spot, chunk(at)] = total.astype(BF16)
            final(at).start()
        for at in range(PIECES):
            final(at).wait_recv()
            spot = outer * 2 + inner
            part[spot, chunk(at)] = add(part[spot, chunk(at)], final_in[chunk(at)])

            @pl.when(section > 0)
            def _(at=at):
                shift(part.at[outer * 2 + inner, chunk(at)], at).start()

    for away in range(1, count):
        p_copy(away).wait_recv()
    total = jnp.zeros((top, tokens), F32)
    for expert in range(experts * count):
        value = prob_in[expert // experts, expert % experts]
        total = jnp.where(ids[...] == expert, value, total)
    prob_out[...] = total.astype(BF16)
    weight_finish()

    for away in range(1, count):
        s_copy(away).wait_send()
        p_copy(away).wait_send()
    for at in range(3):
        o_copy(at).wait_send()

    def drain(step, carry):
        for side in side_list:
            for at in range(4):
                pl.when(leaves(step, side))(z_copy(at, side, step).wait_send)
            for at in range(2):
                pl.when(arrives(step, side))(y_copy(at, side, step).wait_send)
        return carry

    lax.fori_loop(0, line - 1, drain, 0)
    for at in range(PIECES):
        cross(far, far_end, at).wait_send()
        cross(near, near_end, at).wait_send()
        end_copy(far_end, at, far_side).wait_send()

        @pl.when(jnp.logical_not(at_end))
        def _(at=at):
            end_copy(near_end, at, near_side).wait_send()
            final(at).wait_send()

    for block_at in range(1, line - 1):
        for side in side_list:
            @pl.when(block_at > outer if side == 0 else block_at < outer)
            def _(block_at=block_at, side=side):
                for at in range(PIECES):
                    for row in range(2):
                        chain(block_at, side, row, at, hop_of(side)).wait_send()

    @pl.when(section > 0)
    def _():
        for at in range(PIECES):
            shift(end_sum.at[0, chunk(at)], at).wait_send()

    @pl.when(section < sections - 1)
    def _():
        for at in range(PIECES):
            shift(end_sum.at[0, chunk(at)], at).wait_recv()

    @pl.when(section == sections - 1)
    def _():
        out[...] = jnp.zeros_like(out)


def fused(count, sections, g, x, ids, probs, counts, gate_w, up_w, down_w, held, gate, up):
    line = count // 2
    tokens, width = g.shape
    experts, _, hidden = gate_w.shape
    top = ids.shape[0]
    slot_rows = held.shape[1]
    cap = slot_rows // count
    padded = -(-cap // 16) * 16
    dma = pltpu.SemaphoreType.DMA
    roomy = is_roomy(count, tokens, width)
    stage = (1, 16, 128) if roomy else (2, width, hidden)
    results = [(tokens, width), (top, tokens), (experts, width, hidden), (experts, width, hidden)]
    return pl.pallas_call(
        functools.partial(fused_kernel, count, sections, cap, roomy),
        out_shape=[
            pltpu.VMEM(shape, BF16) if roomy else jax.ShapeDtypeStruct(shape, BF16)
            for shape in results
        ],
        in_specs=[HBM, HBM, VMEM, VMEM, SMEM] + [HBM] * 6,
        out_specs=[VMEM, VMEM] + [VMEM if roomy else HBM] * 2,
        scratch_shapes=[
            pltpu.VMEM((count, tokens, width), BF16),
            pltpu.VMEM((count, tokens, width), BF16),
            pltpu.VMEM((count, 2 * top, tokens), BF16),
            pltpu.VMEM((experts, width, 2 * hidden), BF16),
            pltpu.VMEM((experts, hidden, width), BF16),
            pltpu.VMEM((2, slot_rows, width), BF16),
            pltpu.VMEM((2, slot_rows, hidden), BF16),
            pltpu.VMEM((2, slot_rows, hidden), BF16),
            pltpu.VMEM(stage, BF16),
            pltpu.VMEM(stage, BF16),
            pltpu.VMEM((count, experts, 1, tokens), F32),
            pltpu.VMEM((count, experts, 1, tokens), F32),
            pltpu.VMEM((experts, 2 * padded, width), BF16),
            pltpu.VMEM((2, experts, 2 * padded, hidden), F32),
            pltpu.VMEM((2, experts, 2 * padded, hidden), F32),
            pltpu.VMEM((2, experts, 2 * padded, hidden), F32),
            pltpu.VMEM((2, experts * padded, width), BF16),
            pltpu.VMEM((count, tokens, width), BF16),
            pltpu.VMEM((count, experts, 1, tokens), F32),
            pltpu.VMEM((count, experts, 1, tokens), F32),
            pltpu.VMEM((line - 1, 2, tokens, width), BF16),
            pltpu.VMEM((2, tokens, width), BF16),
            pltpu.VMEM((2, tokens, width), BF16),
            pltpu.VMEM((2, tokens, width), BF16),
            pltpu.VMEM((tokens, width), BF16),
            dma((2,)),
            dma((3,)),
            dma((3, 2)),
            dma((2, 2)),
            dma((count - 1,)),
            dma((count - 1,)),
            dma((4, 2, line - 1)),
            dma((4, 2, line - 1)),
            dma((2, 2, line - 1)),
            dma((2, 2, line - 1)),
            dma((3,)),
            dma((3,)),
            dma((count - 1,)),
            dma((count - 1,)),
            dma((line - 2, 2, 2, PIECES)),
            dma((line - 2, 2, 2, PIECES)),
            dma((2, PIECES)),
            dma((2, PIECES)),
            dma((2, PIECES)),
            dma((2, PIECES)),
            dma((PIECES,)),
            dma((PIECES,)),
            dma((PIECES,)),
            dma((PIECES,)),
        ],
        compiler_params=pltpu.CompilerParams(
            collective_id=0, has_side_effects=True,
            vmem_limit_bytes=(48 if roomy else 63) * 1024 * 1024,
        ),
    )(g, x, ids, probs, counts, gate_w, up_w, down_w, held, gate, up)


def is_roomy(count, tokens, width):
    return count * tokens * width <= 2 * 1024 * 1024


def publish(direct, arrays):
    total = len(arrays)

    def kernel(*refs):
        sources, goals, held = refs[:total], refs[total : 2 * total], refs[2 * total : -2]
        read, write = refs[-2:]
        moves = []
        for source, goal, spot in zip(sources, goals, held):
            if len(source.shape) == 2:
                moves.append((source, goal, spot))
        for at in range(sources[-1].shape[0]):
            for source, goal, spot in zip(sources, goals, held):
                if len(source.shape) == 3:
                    moves.append((source.at[at], goal.at[at], spot.at[at]))
        def move(at, source, goal, sems):
            return pltpu.make_async_copy(source, goal, sems.at[at])

        for at, (source, goal, spot) in enumerate(moves):
            if direct:
                move(at, source, goal, write).start()
            else:
                move(at, source, spot, read).start()
        for at, (source, goal, spot) in enumerate(moves):
            if not direct:
                move(at, source, spot, read).wait()
                move(at, spot, goal, write).start()
        for at, (source, goal, spot) in enumerate(moves):
            move(at, source if direct else spot, goal, write).wait()

    pieces = sum(a.shape[0] if len(a.shape) == 3 else 1 for a in arrays)
    return pl.pallas_call(
        kernel,
        out_shape=[jax.ShapeDtypeStruct(a.shape, a.dtype) for a in arrays],
        in_specs=[VMEM if direct else ANY] * total,
        out_specs=[HBM] * total,
        scratch_shapes=[
            pltpu.VMEM((8,) * (len(a.shape) - 1) + (128,) if direct else a.shape, a.dtype)
            for a in arrays
        ]
        + [pltpu.SemaphoreType.DMA((pieces,))] * 2,
        compiler_params=pltpu.CompilerParams(vmem_limit_bytes=(4 if direct else 32) * 1024 * 1024),
    )(*arrays)


def per_device(
    output_grad,
    layer_input,
    expert_ids,
    route_probs,
    gate_weight,
    up_weight,
    down_weight,
    saved_inputs,
    saved_gate_grad,
    saved_up_grad,
    saved_counts,
):
    upstream, prob, gate_part, up_part = fused(
        lax.axis_size("ep"),
        lax.axis_size("section"),
        output_grad[0],
        layer_input[0],
        expert_ids[0].T,
        route_probs[0].T,
        saved_counts[0],
        gate_weight[0],
        up_weight[0],
        down_weight[0],
        saved_inputs[0],
        saved_gate_grad[0],
        saved_up_grad[0],
    )
    direct = is_roomy(lax.axis_size("ep"), output_grad.shape[1], output_grad.shape[2])
    upstream, prob, gate_part, up_part = publish(direct, (upstream, prob, gate_part, up_part))
    return (upstream[None], prob.T[None], gate_part[None], up_part[None])


def solution(mesh):
    three = P("section", "ep", None)
    four = P("section", "ep", None, None)
    return jax.shard_map(
        per_device,
        mesh=mesh,
        in_specs=(three, three, three, three, four, four, four, four, four, four, three),
        out_specs=(three, three, four, four),
        check_vma=False,
    )
```

```python
import functools

import jax
import jax.numpy as jnp
from jax import lax
from jax.experimental import pallas as pl
from jax.experimental.pallas import tpu as pltpu
from jax.sharding import PartitionSpec as P

F32 = jnp.float32
BF16 = jnp.bfloat16
MESH = pl.DeviceIdType.MESH
VMEM = pl.BlockSpec(memory_space=pltpu.VMEM)
SMEM = pl.BlockSpec(memory_space=pltpu.SMEM)
ANY = pl.BlockSpec(memory_space=pl.ANY)
HBM = pl.BlockSpec(memory_space=pltpu.HBM)
TILE = 256
PIECES = 4


def guarded(when, act):
    if when is None:
        act()
    else:
        pl.when(when)(act)


def both(a, b):
    return jnp.logical_and(a, b)


def add(a, b):
    return (a.astype(F32) + b.astype(F32)).astype(BF16)


def dot(a, b, dims):
    return lax.dot_general(a, b, (dims, ((), ())), preferred_element_type=F32)


def cut_of(width):
    return max(width * 4 // 1024, 1) * 128


def fused_kernel(
    count, sections, cap, roomy,
    g, x, ids, probs, counts, gate_w, up_w, down_w, held_in, gate_in, up_in,
    out, prob_out, gate_out, up_out,
    x_all, g_all, s_all, w_in, w_down, held, gate_held, up_held, gate_stage, up_stage,
    slots, weights, rows, keep_hidden, keep_active, keep_gate, back, part, prob_part, prob_in,
    chain_in, cross_in, end_in, end_sum, final_in,
    own_sem, load_sem, held_sem, stage_sem, s_send, s_recv, z_send, z_recv, y_send, y_recv,
    o_send, o_recv, p_send, p_recv, chain_send, chain_recv, cross_send, cross_recv, end_send,
    end_recv, final_send, final_recv, shift_send, shift_recv,
):
    me = lax.axis_index("ep")
    section = lax.axis_index("section")
    outer, inner = me // 2, me % 2
    other = 1 - inner
    line = count // 2
    up = ((outer + 1) % line) * 2 + inner
    down = ((outer + line - 1) % line) * 2 + inner
    sides = (up, down)
    partner = outer * 2 + other
    experts = gate_w.shape[0]
    tokens, width = g.shape
    hidden = gate_w.shape[2]
    top = ids.shape[0]
    padded = rows.shape[1] // 2
    slot_rows = held_in.shape[1]
    cut = cut_of(width)
    everything, few, many = pl.ds(0, width), pl.ds(0, cut), pl.ds(cut, width - cut)
    side_list = (0, 1)

    def remote(src, dst, send, recv, target):
        return pltpu.make_async_remote_copy(
            src_ref=src, dst_ref=dst, send_sem=send, recv_sem=recv, device_id=target,
            device_id_type=MESH,
        )

    own = [
        pltpu.make_async_copy(g, g_all.at[me], own_sem.at[0]),
        pltpu.make_async_copy(x, x_all.at[me], own_sem.at[1]),
    ]
    for copy in own:
        copy.start()

    def held_loads(expert, at):
        return [
            pltpu.make_async_copy(src.at[expert], dst.at[at], held_sem.at[kind, at])
            for kind, (src, dst) in enumerate(
                ((held_in, held), (gate_in, gate_held), (up_in, up_held))
            )
        ]

    s_all[me] = jnp.concatenate([ids[...].astype(F32), probs[...].astype(F32)], axis=0).astype(BF16)

    barrier = pltpu.get_barrier_semaphore()
    for away in range(1, count):
        pl.semaphore_signal(
            barrier, inc=1, device_id={"ep": (me + away) % count}, device_id_type=MESH
        )
    for away in (1, sections - 1):
        pl.semaphore_signal(
            barrier, inc=1, device_id={"section": (section + away) % sections}, device_id_type=MESH
        )
    pl.semaphore_wait(barrier, count + 1)

    def s_copy(away):
        return remote(
            s_all.at[me], s_all.at[me], s_send.at[away - 1], s_recv.at[away - 1],
            {"ep": (me + away) % count},
        )

    for away in range(1, count):
        s_copy(away).start()

    def block(step, side):
        return (outer + (-step if side == 0 else step) + 2 * line) % line

    def arrives(step, side):
        return outer >= step + 1 if side == 0 else outer + step + 1 <= line - 1

    def leaves(step, side):
        if side == 0:
            return both(outer >= step, outer < line - 1)
        return both(outer + step <= line - 1, outer > 0)

    pieces = ((x_all, everything), (g_all, many), (g_all, few), (g_all, few))

    def z_copy(at, side, step, source=None):
        ref, columns = pieces[at]
        spot = ref.at[block(step, side) * 2 + (other if at == 3 else inner), :, columns]
        return remote(
            spot if source is None else source.at[:, columns], spot, z_send.at[at, side, step],
            z_recv.at[at, side, step], {"ep": sides[side]},
        )

    def y_copy(at, side, step):
        ref, columns = pieces[at]
        spot = ref.at[block(step + 1, side) * 2 + inner, :, columns]
        return remote(
            spot, spot, y_send.at[at, side, step], y_recv.at[at, side, step], {"ep": partner}
        )

    def o_copy(at):
        ref, columns = pieces[at]
        spot = ref.at[me, :, columns]
        return remote(
            (x, g, g)[at].at[:, columns], spot, o_send.at[at], o_recv.at[at], {"ep": partner}
        )

    o_copy(2).start()
    for at in range(3):
        for side in side_list:
            pl.when(leaves(0, side))(z_copy(at, side, 0, (x, g, g)[at]).start)
    o_copy(0).start()
    o_copy(1).start()
    for expert in range(min(2, experts)):
        for copy in held_loads(expert, expert):
            copy.start()
    loads = [
        pltpu.make_async_copy(gate_w, w_in.at[:, :, pl.ds(0, hidden)], load_sem.at[0]),
        pltpu.make_async_copy(up_w, w_in.at[:, :, pl.ds(hidden, hidden)], load_sem.at[1]),
        pltpu.make_async_copy(down_w, w_down, load_sem.at[2]),
    ]
    for copy in loads:
        copy.start()


    def hop_of(side):
        return outer + 1 if side == 0 else outer - 1

    def chain(block_at, side, row, at, where):
        rows_at = pl.ds(at * (tokens // PIECES), tokens // PIECES)
        spot = jnp.where(block_at == where, line - 2, block_at - 1) if side == 1 else block_at - 1
        return remote(
            part.at[block_at * 2 + row, rows_at], chain_in.at[spot, row, rows_at],
            chain_send.at[block_at - 1, side, row, at], chain_recv.at[block_at - 1, side, row, at],
            {"ep": sides[side]},
        )

    def weight_expert(expert, carry):
        at = expert % 2
        for copy in held_loads(expert, at):
            copy.wait()
        place = lax.broadcasted_iota(jnp.int32, (slot_rows, 128), 0)
        live = jnp.zeros((slot_rows, 128), F32)
        for source in range(count):
            low = source * cap
            inside = both(place >= low, place < low + counts[expert, source])
            live = jnp.where(inside, 1.0, live)
        live = live.astype(BF16)
        for ref in (gate_held, up_held):
            for group in range(hidden // 128):
                columns = pl.ds(group * 128, 128)
                ref[at, :, columns] = ref[at, :, columns] * live

        def stage_copies(old):
            return [
                pltpu.make_async_copy(stage.at[at], dst.at[old], stage_sem.at[kind, at])
                for kind, (stage, dst) in enumerate(((gate_stage, gate_out), (up_stage, up_out)))
            ]

        if not roomy:
            @pl.when(expert >= 2)
            def _():
                for copy in stage_copies(expert - 2):
                    copy.wait()

        goals = (gate_out, up_out) if roomy else (gate_stage, up_stage)
        place_at = expert if roomy else at

        def body(tile, carry):
            columns = pl.ds(pl.multiple_of(tile * TILE, TILE), TILE)
            some = held[at, :, columns]
            for ref, stage in zip((gate_held, up_held), goals):
                stage[place_at, columns, :] = dot(some, ref[at], ((0,), (0,))).astype(BF16)
            return carry

        lax.fori_loop(0, width // TILE, body, 0)
        if not roomy:
            for copy in stage_copies(expert):
                copy.start()

        @pl.when(expert + 2 < experts)
        def _():
            for copy in held_loads(expert + 2, at):
                copy.start()

        return carry

    def weight_finish():
        if roomy:
            return
        for expert in range(max(experts - 2, 0), experts):
            for kind, (stage, dst) in enumerate(((gate_stage, gate_out), (up_stage, up_out))):
                pltpu.make_async_copy(
                    stage.at[expert % 2], dst.at[expert], stage_sem.at[kind, expert % 2]
                ).wait()

    def route():
        members = []
        for source in range(count):
            named = s_all[source].astype(F32)
            chosen, prob = named[:top], named[top:]
            for expert in range(experts):
                hit = chosen == (me * experts + expert).astype(F32)
                members.append(jnp.max(jnp.where(hit, 1.0, 0.0), axis=0, keepdims=True))
                weights[source, expert] = jnp.sum(jnp.where(hit, prob, 0.0), axis=0, keepdims=True)
        member = jnp.concatenate(members, axis=0)
        earlier = lax.broadcasted_iota(jnp.int32, (tokens, tokens), 0) < lax.broadcasted_iota(
            jnp.int32, (tokens, tokens), 1
        )
        before = dot(
            member.astype(BF16), jnp.where(earlier, 1.0, 0.0).astype(BF16), ((1,), (0,))
        )
        slot = jnp.where(member > 0.5, before, -1.0)
        for source in range(count):
            for expert in range(experts):
                at = source * experts + expert
                slots[source, expert] = slot[at : at + 1]

    spots = lax.broadcasted_iota(jnp.int32, (padded, tokens), 0).astype(F32)

    def picked(source, scaled):
        parts = []
        for expert in range(experts):
            value = weights[source, expert] if scaled else 1.0
            parts.append(jnp.where(spots == slots[source, expert], value, 0.0).astype(BF16))
        return jnp.concatenate(parts, axis=0)

    def spread(unit, ref):
        for row in range(2):
            source = unit * 2 + row
            pick = picked(source, False)
            for tile in range(width // TILE):
                columns = pl.ds(tile * TILE, TILE)
                got = dot(pick, ref[source, :, columns], ((1,), (0,))).astype(BF16)
                for expert in range(experts):
                    rows[expert, pl.ds(row * padded, padded), columns] = got[
                        expert * padded : (expert + 1) * padded
                    ]

    def forward(unit, side):
        spread(unit, x_all)

        def body(expert, carry):
            pre = dot(rows[expert], w_in[expert], ((1,), (0,)))
            gate, upper = pre[:, :hidden], pre[:, hidden:]
            sigma = jax.nn.sigmoid(gate)
            active = gate * sigma
            keep_active[side, expert] = active
            keep_hidden[side, expert] = active * upper
            keep_gate[side, expert] = upper * sigma * (1.0 + gate * (1.0 - sigma))
            return carry

        lax.fori_loop(0, experts, body, 0)

    def backward(unit, side):
        spread(unit, g_all)

        def body(expert, carry):
            grad = dot(rows[expert], w_down[expert], ((1,), (1,)))
            score = jnp.sum(grad * keep_hidden[side, expert], axis=1, keepdims=True)
            score = score.astype(BF16).astype(F32)
            pre_grad = jnp.concatenate(
                [
                    (grad * keep_gate[side, expert]).astype(BF16),
                    (grad * keep_active[side, expert]).astype(BF16),
                ],
                axis=1,
            )
            for tile in range(width // TILE):
                columns = pl.ds(tile * TILE, TILE)
                sent = dot(pre_grad, w_in[expert, columns, :], ((1,), (1,))).astype(BF16)
                for row in range(2):
                    back[
                        row, pl.ds(pl.multiple_of(expert * padded, padded), padded), columns
                    ] = sent[row * padded : (row + 1) * padded]
            for row in range(2):
                source = unit * 2 + row
                mine = jnp.where(
                    spots == slots[source, expert], score[row * padded : (row + 1) * padded], 0.0
                )
                prob_part[source, expert] = jnp.sum(mine, axis=0, keepdims=True)
            return carry

        lax.fori_loop(0, experts, body, 0)
        for row in range(2):
            source = unit * 2 + row
            put = picked(source, True)
            for tile in range(width // TILE):
                columns = pl.ds(tile * TILE, TILE)
                sent = dot(put, back[row, :, columns], ((0,), (0,)))
                part[source, :, columns] = sent.astype(BF16)
        within = both(unit > 0, unit < line - 1)
        for way, edge in ((0, 0), (1, line - 1)):
            @pl.when(both(outer == edge, within))
            def _(way=way, edge=edge):
                split = unit == (line - 2 if edge == 0 else 1)
                for at in range(PIECES):
                    for row in range(2):
                        send = chain(unit, way, row, at, hop_of(way)).start
                        if at < PIECES // 2:
                            send()
                        else:
                            pl.when(jnp.logical_not(split))(send)

    def unit_turn(step, side, act, at):
        unit = (outer + (-step - 1 if side == 0 else step + 1) + 2 * line) % line
        own_turn = step < 0
        later = both(arrives(step, side), step >= 0)
        pl.when(later)(y_copy(at, side, step).wait_recv)
        if side == 0:
            pl.when(own_turn)(o_copy(at).wait_recv)

        @pl.when(jnp.logical_or(later, own_turn) if side == 0 else later)
        def _():
            act(unit, side)

    def take(at, step):
        for side in side_list:
            pl.when(arrives(step, side))(z_copy(at, side, step).wait_recv)

            @pl.when(both(leaves(step + 1, side), step < line - 2))
            def _(side=side):
                z_copy(at, side, step + 1).start()

            if at < 2:
                pl.when(arrives(step, side))(y_copy(at, side, step).start)

    at_end = jnp.logical_or(outer == 0, outer == line - 1)

    def turn(index, carry):
        step = index - 1
        early = both(step >= 0, step < line - 2)
        pl.when(early)(lambda: take(0, step))
        pl.when(both(early, index == 1))(lambda: take(1, step))

        @pl.when(index < 2)
        def _():
            experts_of(index)

        @pl.when(step >= 0)
        def _():
            unit_turn(step - 1, 0, backward, 1)
            unit_turn(step - 1, 1, backward, 1)

        pl.when(both(early, index > 1))(lambda: take(1, step))

        @pl.when(index >= 2)
        def _():
            experts_of(index)

        @pl.when(step == line - 2)
        def _():
            take(0, step)
            take(1, step)
            chain_start(range(PIECES // 2, PIECES))

        @pl.when(early)
        def _():
            take(2, step)
            take(3, step)

        @pl.when(step < line - 1)
        def _():
            unit_turn(step, 0, forward, 0)
            unit_turn(step, 1, forward, 0)

        @pl.when(step == line - 2)
        def _():
            take(2, step)
            take(3, step)

        return carry

    def experts_of(index):
        first = jnp.where(index == 0, 0, jnp.minimum(index + 1, experts))
        last = jnp.minimum(index + 2, experts)
        lax.fori_loop(first, last, weight_expert, 0)

    def chain_start(some):
        for way, edge, unit in ((0, 0, line - 2), (1, line - 1, 1)):
            @pl.when(outer == edge)
            def _(way=way, unit=unit):
                for at in some:
                    for row in range(2):
                        chain(unit, way, row, at, hop_of(way)).start()

    for away in range(1, count):
        s_copy(away).wait_recv()
    route()
    for copy in own:
        copy.wait()
    o_copy(2).wait_recv()
    for side in side_list:
        pl.when(leaves(0, side))(z_copy(3, side, 0).start)
    for copy in loads:
        copy.wait()
    lax.fori_loop(0, line + 1, turn, 0)
    if experts > line + 2:
        lax.fori_loop(line + 2, experts, weight_expert, 0)

    span = tokens // PIECES
    far = jnp.where(outer < line // 2, line - 1, 0)
    near = line - 1 - far
    far_end, near_end = far // (line - 1), near // (line - 1)
    far_side = jnp.where(outer < line // 2, up, down)
    near_side = jnp.where(outer < line // 2, down, up)

    def chunk(at):
        return pl.ds(at * span, span)

    def p_copy(away):
        target = (me + away) % count
        return remote(
            prob_part.at[target], prob_in.at[me], p_send.at[away - 1], p_recv.at[away - 1],
            {"ep": target},
        )

    def cross(block_at, end, at):
        return remote(
            part.at[block_at * 2 + other, chunk(at)], cross_in.at[end, chunk(at)],
            cross_send.at[end, at], cross_recv.at[end, at], {"ep": partner},
        )

    def final(at):
        return remote(
            part.at[outer * 2 + other, chunk(at)], final_in.at[chunk(at)], final_send.at[at],
            final_recv.at[at], {"ep": partner},
        )

    def end_copy(end, at, target):
        return remote(
            end_sum.at[end, chunk(at)], end_in.at[end, chunk(at)], end_send.at[end, at],
            end_recv.at[end, at], {"ep": target},
        )

    def shift(source, at):
        return remote(
            source, out.at[chunk(at)], shift_send.at[at], shift_recv.at[at],
            {"section": (section + sections - 1) % sections},
        )

    for away in range(1, count):
        p_copy(away).start()
    prob_in[me] = prob_part[me]
    ends = ((far, far_end), (near, near_end))
    in_turn = [(end, at) for end in range(2) for at in range(PIECES)]
    mixed_up = [(end, at) for at in range(PIECES) for end in range(2)]

    def crossing(order):
        for end, piece in order:
            cross(*ends[end], piece).start()

    def end_step(order, place, target):
        is_far, at = order[place][0] == 0, order[place][1]
        block_at, end = ends[order[place][0]]
        cross(block_at, end, at).wait_recv()
        rows_at = chunk(at)
        total = part[block_at * 2 + inner, rows_at].astype(F32) + cross_in[end, rows_at].astype(F32)
        end_sum[end, rows_at] = total.astype(BF16)
        first = jnp.logical_or(outer == 0, outer == line - 1) if is_far else None

        def gather_in():
            end_copy(end, at, target).wait_recv()
            end_sum[end, rows_at] = add(end_sum[end, rows_at], end_in[end, rows_at])

        if is_far:
            pl.when(jnp.logical_not(first))(gather_in)
            end_copy(end, at, target).start()
        else:
            gather_in()

    @pl.when(at_end)
    def _():
        crossing(in_turn[:PIECES])
        for at in range(PIECES):
            end_step(in_turn, at, far_side)
        crossing(in_turn[PIECES:])
        for at in range(PIECES):
            end_step(in_turn, PIECES + at, near_side)

            @pl.when(section > 0)
            def _(at=at):
                shift(end_sum.at[near_end, chunk(at)], at).start()

    @pl.when(jnp.logical_not(at_end))
    def _():
        crossing(mixed_up)
        order = []
        for half in range((line - 1) // 2):
            order += [line - 2 - half] + ([1 + half] if 1 + half != line - 2 - half else [])
        for block_at in order:
            for side in side_list:
                @pl.when(block_at > outer if side == 0 else block_at < outer)
                def _(block_at=block_at, side=side):
                    for at in range(PIECES):
                        for row in range(2):
                            chain(block_at, side, row, at, outer).wait_recv()
                            spot = block_at * 2 + row
                            part[spot, chunk(at)] = add(
                                part[spot, chunk(at)], chain_in[block_at - 1, row, chunk(at)]
                            )
                            chain(block_at, side, row, at, hop_of(side)).start()
        for at in range(PIECES):
            end_step(mixed_up, 2 * at, far_side)
            end_step(mixed_up, 2 * at + 1, near_side)
            end_copy(near_end, at, near_side).start()
            for row in range(2):
                for side in side_list:
                    chain(outer, side, row, at, outer).wait_recv()
                spot = outer * 2 + row
                total = part[spot, chunk(at)].astype(F32)
                total = total + chain_in[outer - 1, row, chunk(at)].astype(F32)
                total = total + chain_in[line - 2, row, chunk(at)].astype(F32)
                part[spot, chunk(at)] = total.astype(BF16)
            final(at).start()
        for at in range(PIECES):
            final(at).wait_recv()
            spot = outer * 2 + inner
            part[spot, chunk(at)] = add(part[spot, chunk(at)], final_in[chunk(at)])

            @pl.when(section > 0)
            def _(at=at):
                shift(part.at[outer * 2 + inner, chunk(at)], at).start()

    for away in range(1, count):
        p_copy(away).wait_recv()
    total = jnp.zeros((top, tokens), F32)
    for expert in range(experts * count):
        value = prob_in[expert // experts, expert % experts]
        total = jnp.where(ids[...] == expert, value, total)
    prob_out[...] = total.astype(BF16)
    weight_finish()

    for away in range(1, count):
        s_copy(away).wait_send()
        p_copy(away).wait_send()
    for at in range(3):
        o_copy(at).wait_send()

    def drain(step, carry):
        for side in side_list:
            for at in range(4):
                pl.when(leaves(step, side))(z_copy(at, side, step).wait_send)
            for at in range(2):
                pl.when(arrives(step, side))(y_copy(at, side, step).wait_send)
        return carry

    lax.fori_loop(0, line - 1, drain, 0)
    for at in range(PIECES):
        cross(far, far_end, at).wait_send()
        cross(near, near_end, at).wait_send()
        end_copy(far_end, at, far_side).wait_send()

        @pl.when(jnp.logical_not(at_end))
        def _(at=at):
            end_copy(near_end, at, near_side).wait_send()
            final(at).wait_send()

    for block_at in range(1, line - 1):
        for side in side_list:
            @pl.when(block_at > outer if side == 0 else block_at < outer)
            def _(block_at=block_at, side=side):
                for at in range(PIECES):
                    for row in range(2):
                        chain(block_at, side, row, at, hop_of(side)).wait_send()

    @pl.when(section > 0)
    def _():
        for at in range(PIECES):
            shift(end_sum.at[0, chunk(at)], at).wait_send()

    @pl.when(section < sections - 1)
    def _():
        for at in range(PIECES):
            shift(end_sum.at[0, chunk(at)], at).wait_recv()

    @pl.when(section == sections - 1)
    def _():
        out[...] = jnp.zeros_like(out)


def fused(count, sections, g, x, ids, probs, counts, gate_w, up_w, down_w, held, gate, up):
    line = count // 2
    tokens, width = g.shape
    experts, _, hidden = gate_w.shape
    top = ids.shape[0]
    slot_rows = held.shape[1]
    cap = slot_rows // count
    padded = -(-cap // 16) * 16
    dma = pltpu.SemaphoreType.DMA
    roomy = is_roomy(count, tokens, width)
    stage = (1, 16, 128) if roomy else (2, width, hidden)
    results = [(tokens, width), (top, tokens), (experts, width, hidden), (experts, width, hidden)]
    return pl.pallas_call(
        functools.partial(fused_kernel, count, sections, cap, roomy),
        out_shape=[
            pltpu.VMEM(shape, BF16) if roomy else jax.ShapeDtypeStruct(shape, BF16)
            for shape in results
        ],
        in_specs=[HBM, HBM, VMEM, VMEM, SMEM] + [HBM] * 6,
        out_specs=[VMEM, VMEM] + [VMEM if roomy else HBM] * 2,
        scratch_shapes=[
            pltpu.VMEM((count, tokens, width), BF16),
            pltpu.VMEM((count, tokens, width), BF16),
            pltpu.VMEM((count, 2 * top, tokens), BF16),
            pltpu.VMEM((experts, width, 2 * hidden), BF16),
            pltpu.VMEM((experts, hidden, width), BF16),
            pltpu.VMEM((2, slot_rows, width), BF16),
            pltpu.VMEM((2, slot_rows, hidden), BF16),
            pltpu.VMEM((2, slot_rows, hidden), BF16),
            pltpu.VMEM(stage, BF16),
            pltpu.VMEM(stage, BF16),
            pltpu.VMEM((count, experts, 1, tokens), F32),
            pltpu.VMEM((count, experts, 1, tokens), F32),
            pltpu.VMEM((experts, 2 * padded, width), BF16),
            pltpu.VMEM((2, experts, 2 * padded, hidden), F32),
            pltpu.VMEM((2, experts, 2 * padded, hidden), F32),
            pltpu.VMEM((2, experts, 2 * padded, hidden), F32),
            pltpu.VMEM((2, experts * padded, width), BF16),
            pltpu.VMEM((count, tokens, width), BF16),
            pltpu.VMEM((count, experts, 1, tokens), F32),
            pltpu.VMEM((count, experts, 1, tokens), F32),
            pltpu.VMEM((line - 1, 2, tokens, width), BF16),
            pltpu.VMEM((2, tokens, width), BF16),
            pltpu.VMEM((2, tokens, width), BF16),
            pltpu.VMEM((2, tokens, width), BF16),
            pltpu.VMEM((tokens, width), BF16),
            dma((2,)),
            dma((3,)),
            dma((3, 2)),
            dma((2, 2)),
            dma((count - 1,)),
            dma((count - 1,)),
            dma((4, 2, line - 1)),
            dma((4, 2, line - 1)),
            dma((2, 2, line - 1)),
            dma((2, 2, line - 1)),
            dma((3,)),
            dma((3,)),
            dma((count - 1,)),
            dma((count - 1,)),
            dma((line - 2, 2, 2, PIECES)),
            dma((line - 2, 2, 2, PIECES)),
            dma((2, PIECES)),
            dma((2, PIECES)),
            dma((2, PIECES)),
            dma((2, PIECES)),
            dma((PIECES,)),
            dma((PIECES,)),
            dma((PIECES,)),
            dma((PIECES,)),
        ],
        compiler_params=pltpu.CompilerParams(
            collective_id=0, has_side_effects=True,
            vmem_limit_bytes=(48 if roomy else 63) * 1024 * 1024,
        ),
    )(g, x, ids, probs, counts, gate_w, up_w, down_w, held, gate, up)


def is_roomy(count, tokens, width):
    return count * tokens * width <= 2 * 1024 * 1024


def publish(direct, arrays):
    total = len(arrays)

    def kernel(*refs):
        sources, goals, held = refs[:total], refs[total : 2 * total], refs[2 * total : -2]
        read, write = refs[-2:]
        moves = []
        for source, goal, spot in zip(sources, goals, held):
            if len(source.shape) == 2:
                moves.append((source, goal, spot))
        for at in range(sources[-1].shape[0]):
            for source, goal, spot in zip(sources, goals, held):
                if len(source.shape) == 3:
                    moves.append((source.at[at], goal.at[at], spot.at[at]))
        def move(at, source, goal, sems):
            return pltpu.make_async_copy(source, goal, sems.at[at])

        for at, (source, goal, spot) in enumerate(moves):
            if direct:
                move(at, source, goal, write).start()
            else:
                move(at, source, spot, read).start()
        for at, (source, goal, spot) in enumerate(moves):
            if not direct:
                move(at, source, spot, read).wait()
                move(at, spot, goal, write).start()
        for at, (source, goal, spot) in enumerate(moves):
            move(at, source if direct else spot, goal, write).wait()

    pieces = sum(a.shape[0] if len(a.shape) == 3 else 1 for a in arrays)
    return pl.pallas_call(
        kernel,
        out_shape=[jax.ShapeDtypeStruct(a.shape, a.dtype) for a in arrays],
        in_specs=[VMEM if direct else ANY] * total,
        out_specs=[HBM] * total,
        scratch_shapes=[
            pltpu.VMEM((8,) * (len(a.shape) - 1) + (128,) if direct else a.shape, a.dtype)
            for a in arrays
        ]
        + [pltpu.SemaphoreType.DMA((pieces,))] * 2,
        compiler_params=pltpu.CompilerParams(vmem_limit_bytes=(4 if direct else 32) * 1024 * 1024),
    )(*arrays)


def per_device(
    output_grad,
    layer_input,
    expert_ids,
    route_probs,
    gate_weight,
    up_weight,
    down_weight,
    saved_inputs,
    saved_gate_grad,
    saved_up_grad,
    saved_counts,
):
    upstream, prob, gate_part, up_part = fused(
        lax.axis_size("ep"),
        lax.axis_size("section"),
        output_grad[0],
        layer_input[0],
        expert_ids[0].T,
        route_probs[0].T,
        saved_counts[0],
        gate_weight[0],
        up_weight[0],
        down_weight[0],
        saved_inputs[0],
        saved_gate_grad[0],
        saved_up_grad[0],
    )
    direct = is_roomy(lax.axis_size("ep"), output_grad.shape[1], output_grad.shape[2])
    upstream, prob, gate_part, up_part = publish(direct, (upstream, prob, gate_part, up_part))
    return (upstream[None], prob.T[None], gate_part[None], up_part[None])


def solution(mesh):
    three = P("section", "ep", None)
    four = P("section", "ep", None, None)
    return jax.shard_map(
        per_device,
        mesh=mesh,
        in_specs=(three, three, three, three, four, four, four, four, four, four, three),
        out_specs=(three, three, four, four),
        check_vma=False,
    )
```
